32 devices in a mesh: dom: 4 (over x, core), orient: 8 (over z, y).
Axes of the slice: x: 2, y: 2, z: 4, core: 2. Of those that a mesh axis runs over, the one named last changes fastest.
Arguments:
- particles: bfloat16 [2048, 2, 8192], P(('dom', 'orient')), may hold values from -48 to 48
- templates: bfloat16 [2048, 2, 8192], P('orient'), may hold values from -6 to 6
- tilt_low: int32 [2048], P(('dom', 'orient')), may hold values from 0 to 23
- tilt_high: int32 [2048], P(('dom', 'orient')), may hold values from 40 to 63
Outputs:
- updated: float32 [2048, 2, 8192], P('orient', None, 'dom')
- log_evidence: float32 [2048], P('dom')
The draws below stay inside these ranges and needn't reach their ends.
All inputs are finite; a program needn't handle non-finite values.
Results may differ from the reference program's by a relative error of at most 0.0045.
Values may be sent and summed in bfloat16 or wider, within the bound.
A program may use at most 192 MiB of HBM per device.

```python
import math
import jax
import jax.numpy as jnp
from jax import lax

K = 8192
NBIN = 64
R_DEV = 256
P_GRP = 512
R = 2048
P_SIZE = 2048
N_DOM = 4


def template_values(key):
    template_key = jax.random.fold_in(key, 11)
    return jnp.clip(jax.random.normal(template_key, (R, 2, K), jnp.float32), -6.0, 6.0)


def draw_templates(key, part):
    return template_values(key).astype(jnp.bfloat16)


def draw_particles(key, part):
    noise_key = jax.random.fold_in(key, 23)
    noise_values = jnp.clip(jax.random.normal(noise_key, (P_SIZE, 2, K), jnp.float32), -6.0, 6.0)
    factor = 0.5 + 60.0 / math.sqrt(K)
    chosen_refs = jax.random.randint(jax.random.fold_in(key, 29), (P_SIZE,), 0, R)
    aligned = factor * template_values(key).astype(jnp.bfloat16).astype(jnp.float32)[chosen_refs]
    picked_rows = jnp.arange(P_SIZE) % 16 == 0
    noise_values = jnp.where(picked_rows[:, None, None], aligned, noise_values)
    noise_values = jnp.clip(noise_values, -48.0, 48.0)
    return noise_values.astype(jnp.bfloat16)


def with_ends(entries, rng, smallest, high):
    place = [jax.random.randint(jax.random.fold_in(rng, axis), (), 0, length) for axis, length in enumerate(entries.shape)]
    widest = entries.shape.index(max(entries.shape))
    beside = place[:widest] + [(place[widest] + 1) % entries.shape[widest]] + place[widest + 1:]
    return entries.at[tuple(place)].set(smallest).at[tuple(beside)].set(high)


def setup_inputs(seed: int = 0) -> dict:
    streams_of = jax.random.split(jax.random.key(seed), 5)
    return {
        "particles": draw_particles(jax.random.fold_in(streams_of[4], 71), 0),
        "templates": draw_templates(jax.random.fold_in(streams_of[4], 71), 0),
        "tilt_low": with_ends(jax.random.randint(streams_of[2], (P_SIZE,), 0, 24), jax.random.fold_in(streams_of[2], 1), 0, 23).astype(jnp.int32),
        "tilt_high": with_ends(jax.random.randint(streams_of[3], (P_SIZE,), 40, 64), jax.random.fold_in(streams_of[3], 1), 40, 63).astype(jnp.int32),
    }


def bin_index(band_size):
    return jnp.arange(band_size, dtype=jnp.int32) * 37 % NBIN

def reference(particles, templates, tilt_low, tilt_high):
    inverse_temp = 3.0 / math.sqrt(K)
    binned = bin_index(K)
    observed = ((tilt_low[:, None] <= binned[None, :]) & (binned[None, :] < tilt_high[:, None])).astype(jnp.bfloat16)
    masked = particles * observed[:, None, :]
    flat_rows = masked.reshape(P_SIZE, 2 * K)
    residue_mask = observed[:, :NBIN].astype(jnp.float32)
    blocks = R // R_DEV
    template_blocks = templates.reshape(blocks, R_DEV, 2, K)

    def score_block(template_block):
        template_flat = template_block.reshape(R_DEV, 2 * K)
        correlation = lax.dot_general(flat_rows, template_flat, (((1,), (1,)), ((), ())), preferred_element_type=jnp.float32)
        real_part = template_block[:, 0, :].astype(jnp.float32)
        imag_part = template_block[:, 1, :].astype(jnp.float32)
        power = real_part * real_part + imag_part * imag_part
        residue_power = lax.optimization_barrier(jnp.sum(power.reshape(R_DEV, K // NBIN, NBIN), axis=1))
        penalty = jnp.dot(residue_mask, residue_power.T, precision=lax.Precision.HIGHEST)
        return inverse_temp * (correlation - 0.5 * penalty)
    scores = lax.map(score_block, template_blocks)
    scores = jnp.transpose(scores, (1, 0, 2)).reshape(P_SIZE, R)
    peak_score = lax.optimization_barrier(jnp.max(scores, axis=1))
    total_mass = lax.optimization_barrier(jnp.sum(jnp.exp(scores - peak_score[:, None]), axis=1))
    log_evidence = peak_score + jnp.log(total_mass)
    weights = jnp.exp(scores - log_evidence[:, None]).astype(jnp.bfloat16)
    weight_blocks = jnp.transpose(weights.reshape(P_SIZE, blocks, R_DEV), (1, 0, 2))

    def update_block(inputs):
        weight_block, template_block = inputs
        numerator = jnp.zeros((R_DEV, 2 * K), jnp.float32)
        denominator = jnp.zeros((R_DEV, K), jnp.float32)
        for group_id in range(N_DOM):
            lower = group_id * P_GRP
            group_weights = weight_block[lower:lower + P_GRP]
            part_num = lax.dot_general(group_weights, flat_rows[lower:lower + P_GRP], (((0,), (0,)), ((), ())), preferred_element_type=jnp.float32)
            part_den = lax.dot_general(group_weights, observed[lower:lower + P_GRP], (((0,), (0,)), ((), ())), preferred_element_type=jnp.float32)
            part_num = lax.optimization_barrier(part_num.astype(jnp.bfloat16))
            part_den = lax.optimization_barrier(part_den.astype(jnp.bfloat16))
            numerator = numerator + part_num.astype(jnp.float32)
            denominator = denominator + part_den.astype(jnp.float32)
        numerator = numerator.reshape(R_DEV, 2, K)
        return (numerator + template_block.astype(jnp.float32)) / (denominator[:, None, :] + 1.0)
    updated = lax.map(update_block, (weight_blocks, template_blocks)).reshape(R, 2, K)
    return (updated, log_evidence)
```

```python
import functools
import math

import jax
import jax.numpy as jnp
from jax import lax
from jax.experimental import pallas as pl
from jax.experimental.pallas import tpu as pltpu
from jax.sharding import PartitionSpec as P

NBIN = 64
LANES = 128
MESH = pl.DeviceIdType.MESH


def bin_index(positions):
    return positions * 37 % NBIN


def kernel(
    doms, n, group, scale, xin_ref, t_ref, out_ref, lse_ref,
    x, part, score, stat, stat_all, wts, power,
    own_sem, x_send, x_recv, x_out, part_send, part_recv, stat_send, stat_recv,
):
    dom = lax.axis_index("dom")
    o = lax.axis_index("orient")
    line = n // 2
    a, b = o // 2, o % 2
    mate = a * 2 + (1 - b)
    rows, width = xin_ref.shape[1], xin_ref.shape[2]
    refs, body = t_ref.shape
    groups = n // group
    cols = group * doms * rows
    early = group == 1

    barrier = pltpu.get_barrier_semaphore()

    @pl.loop(1, doms)
    def _(i):
        pl.semaphore_signal(barrier, inc=1, device_id=(lax.rem(dom + i, doms), o), device_id_type=MESH)

    @pl.loop(1, n)
    def _(i):
        pl.semaphore_signal(barrier, inc=1, device_id=(dom, lax.rem(o + i, n)), device_id_type=MESH)

    pl.semaphore_wait(barrier, doms + n - 2)

    def spread(i):
        to = lax.rem(dom + i, doms)
        return pltpu.make_async_remote_copy(
            src_ref=xin_ref.at[to], dst_ref=x.at[o, dom],
            send_sem=x_out.at[i], recv_sem=x_recv.at[o, dom],
            device_id=(to, o), device_id_type=MESH,
        )

    own = pltpu.make_async_copy(xin_ref.at[dom], x.at[o, dom], own_sem)
    own.start()
    for i in range(1, doms):
        spread(i).start()

    def hop(direction, p, d, to):
        return pltpu.make_async_remote_copy(
            src_ref=x.at[p, d], dst_ref=x.at[p, d],
            send_sem=x_send.at[direction, p // 2, d], recv_sem=x_recv.at[p, d],
            device_id=(dom, to), device_id_type=MESH,
        )

    def arrive(p, d):
        hop(0, p, d, mate).wait_recv()

    def right(p, d):
        @pl.when(a + 1 < line)
        def _():
            hop(0, p, d, o + 2).start()

    def left(p, d):
        @pl.when(a > 0)
        def _():
            hop(1, p, d, o - 2).start()

    def across(p, d):
        hop(2, p, d, mate).start()

    def part_copy(g, i):
        return pltpu.make_async_remote_copy(
            src_ref=part.at[dom, g], dst_ref=part.at[dom, g],
            send_sem=part_send.at[i, g], recv_sem=part_recv.at[dom, g],
            device_id=(lax.rem(dom + i, doms), o), device_id_type=MESH,
        )

    def power_of():
        total = jnp.zeros((refs, LANES), jnp.float32)
        for j in range(body // LANES):
            piece = t_ref[:, j * LANES:(j + 1) * LANES].astype(jnp.float32)
            total = total + piece * piece
        total = total * -0.5
        high = total.astype(jnp.bfloat16)
        rest = total - high.astype(jnp.float32)
        middle = rest.astype(jnp.bfloat16)
        low = (rest - middle.astype(jnp.float32)).astype(jnp.bfloat16)
        power[0], power[1], power[2] = high, middle, low

    nt = (((1,), (1,)), ((), ()))

    def scores_of(g):
        block = x[pl.ds(g * group, group)].reshape(cols, width)
        seen = block[:, body:]
        total = lax.dot_general(t_ref[...], block[:, :body], nt, preferred_element_type=jnp.float32)
        for j in range(3):
            total = total + lax.dot_general(power[j], seen, nt, preferred_element_type=jnp.float32)
        part[dom, g] = total
        for i in range(1, doms):
            part_copy(g, i).start()

    power_of()
    own.wait()
    for i in range(doms):
        d = lax.rem(dom + i, doms)
        if i > 0:
            arrive(o, d)
        right(o, d)
        left(o, d)
        across(o, d)
    if early:
        scores_of(o)

    @pl.loop(1, line)
    def _(s):
        for i in range(doms):
            d = lax.rem(dom + i, doms)

            @pl.when(a - s >= 0)
            def _():
                p = o - 2 * s
                arrive(p, d)
                right(p, d)
                across(p, d)

            @pl.when(a + s < line)
            def _():
                p = o + 2 * s
                arrive(p, d)
                left(p, d)
                across(p, d)

        if early:
            for sign in (-1, 1):
                @pl.when((a + sign * s >= 0) & (a + sign * s < line))
                def _():
                    scores_of(o + 2 * sign * s)

    @pl.loop(0, 2 * line - 1)
    def _(j):
        s = (j + 1) // 2
        sign = 1 - 2 * (j % 2)
        at = a + sign * s

        @pl.when((at >= 0) & (at < line))
        def _():
            p = at * 2 + (1 - b)
            for i in range(doms):
                arrive(p, lax.rem(dom + i, doms))
            if early:
                scores_of(p)

    if not early:
        @pl.loop(0, groups)
        def _(g):
            scores_of(g)

    @pl.loop(0, groups)
    def _(g):
        for i in range(1, doms):
            d = lax.rem(dom + i, doms)
            pltpu.make_async_remote_copy(
                src_ref=part.at[d, g], dst_ref=part.at[d, g],
                send_sem=part_send.at[i, g], recv_sem=part_recv.at[d, g],
                device_id=(d, o), device_id_type=MESH,
            ).wait_recv()
        total = part[0, g]
        for d in range(1, doms):
            total = total + part[d, g]
        total = total * scale
        score[g] = total
        peak = jnp.max(total, axis=0, keepdims=True)
        stat[0, pl.ds(g, 1), :] = peak
        stat[1, pl.ds(g, 1), :] = jnp.sum(jnp.exp(total - peak), axis=0, keepdims=True)

    def stat_copy(i):
        return pltpu.make_async_remote_copy(
            src_ref=stat, dst_ref=stat_all.at[o],
            send_sem=stat_send.at[i], recv_sem=stat_recv.at[o],
            device_id=(dom, lax.rem(o + i, n)), device_id_type=MESH,
        )

    @pl.loop(1, n)
    def _(i):
        stat_copy(i).start()

    stat_all[o] = stat[...]

    @pl.loop(1, n)
    def _(i):
        p = lax.rem(o + i, n)
        pltpu.make_async_remote_copy(
            src_ref=stat, dst_ref=stat_all.at[p],
            send_sem=stat_send.at[i], recv_sem=stat_recv.at[p],
            device_id=(dom, p), device_id_type=MESH,
        ).wait_recv()

    top = stat_all[0, 0]
    for p in range(1, n):
        top = jnp.maximum(top, stat_all[p, 0])
    mass = jnp.zeros_like(top)
    for p in range(n):
        mass = mass + stat_all[p, 1] * jnp.exp(stat_all[p, 0] - top)
    lse_ref[...] = top + jnp.log(mass)

    for g in range(groups):
        wts[:, g * cols:(g + 1) * cols] = jnp.exp(score[g] - lse_ref[g:g + 1, :]).astype(jnp.bfloat16)

    nn = (((1,), (0,)), ((), ()))
    seen = x[:, :, :, body:].reshape(n * doms * rows, LANES)
    norm = 1.0 / (lax.dot_general(wts[...], seen, nn, preferred_element_type=jnp.float32) + 1.0)
    tile = 4 * LANES
    norm = jnp.concatenate([norm] * 4, axis=1)

    @pl.loop(0, body // tile)
    def _(j):
        at = pl.ds(pl.multiple_of(j * tile, tile), tile)
        piece = x[:, :, :, at].reshape(n * doms * rows, tile)
        num = lax.dot_general(wts[...], piece, nn, preferred_element_type=jnp.float32)
        out_ref[:, at] = (num + t_ref[:, at].astype(jnp.float32)) * norm

    for i in range(1, doms):
        spread(i).wait_send()

    @pl.loop(0, line)
    def _(q):
        p = q * 2 + b
        for d in range(doms):
            @pl.when((q <= a) & (a + 1 < line))
            def _():
                hop(0, p, d, mate).wait_send()

            @pl.when((q >= a) & (a > 0))
            def _():
                hop(1, p, d, mate).wait_send()

            hop(2, p, d, mate).wait_send()

    @pl.loop(0, groups)
    def _(g):
        for i in range(1, doms):
            part_copy(g, i).wait_send()

    @pl.loop(1, n)
    def _(i):
        stat_copy(i).wait_send()


def on_device(particles, templates, tilt_low, tilt_high):
    doms, n = lax.axis_size("dom"), lax.axis_size("orient")
    rows, _, band = particles.shape
    refs = templates.shape[0]
    part_band = band // doms
    body = 2 * part_band
    width = body + LANES
    group = max(1, 2 * LANES // (doms * rows))
    groups = n // group
    cols = group * doms * rows

    binned = bin_index(jnp.arange(band, dtype=jnp.int32))
    observed = (
        (tilt_low[:, None] <= binned[None, :]) & (binned[None, :] < tilt_high[:, None])
    ).astype(jnp.bfloat16)
    masked = particles * observed[:, None, :]
    masked = masked.reshape(rows, 2, doms, part_band).transpose(2, 0, 1, 3).reshape(doms, rows, body)
    seen = jnp.broadcast_to(observed[None, :, :LANES], (doms, rows, LANES))
    xin = jnp.concatenate([masked, seen], axis=2)
    start = lax.axis_index("dom") * part_band
    t = lax.dynamic_slice_in_dim(templates, start, part_band, 2).reshape(refs, body)

    vmem = pl.BlockSpec(memory_space=pltpu.VMEM)
    updated, lse = pl.pallas_call(
        functools.partial(kernel, doms, n, group, 3.0 / math.sqrt(band)),
        out_shape=(
            jax.ShapeDtypeStruct((refs, body), jnp.float32),
            jax.ShapeDtypeStruct((groups, cols), jnp.float32),
        ),
        in_specs=[vmem, vmem],
        out_specs=(vmem, vmem),
        scratch_shapes=[
            pltpu.VMEM((n, doms, rows, width), jnp.bfloat16),
            pltpu.VMEM((doms, groups, refs, cols), jnp.float32),
            pltpu.VMEM((groups, refs, cols), jnp.float32),
            pltpu.VMEM((2, groups, cols), jnp.float32),
            pltpu.VMEM((n, 2, groups, cols), jnp.float32),
            pltpu.VMEM((refs, n * doms * rows), jnp.bfloat16),
            pltpu.VMEM((3, refs, LANES), jnp.bfloat16),
            pltpu.SemaphoreType.DMA,
            pltpu.SemaphoreType.DMA((3, n // 2, doms)),
            pltpu.SemaphoreType.DMA((n, doms)),
            pltpu.SemaphoreType.DMA((doms,)),
            pltpu.SemaphoreType.DMA((doms, groups)),
            pltpu.SemaphoreType.DMA((doms, groups)),
            pltpu.SemaphoreType.DMA((n,)),
            pltpu.SemaphoreType.DMA((n,)),
        ],
        compiler_params=pltpu.CompilerParams(
            collective_id=0, has_side_effects=True, vmem_limit_bytes=60 * 2**20
        ),
    )(xin, t)
    mine = lax.dynamic_index_in_dim(
        lse.reshape(n, doms, rows), lax.axis_index("dom"), 1, keepdims=False
    )
    return updated.reshape(refs, 2, part_band), mine.reshape(n * rows)


def solution(mesh):
    in_specs = (
        P(("dom", "orient"), None, None),
        P("orient", None, None),
        P(("dom", "orient")),
        P(("dom", "orient")),
    )
    out_specs = (P("orient", None, "dom"), P("dom"))
    return jax.shard_map(
        on_device, mesh=mesh, in_specs=in_specs, out_specs=out_specs, check_vma=False
    )
```

```python
import functools
import math

import jax
import jax.numpy as jnp
from jax import lax
from jax.experimental import pallas as pl
from jax.experimental.pallas import tpu as pltpu
from jax.sharding import PartitionSpec as P

NBIN = 64
LANES = 128
MESH = pl.DeviceIdType.MESH


def bin_index(positions):
    return positions * 37 % NBIN


def kernel(
    doms, n, group, scale, raw_ref, seen_ref, tall_ref, out_ref, lse_ref,
    xin_ref, t_raw, t_ref, x, part, score, stat, stat_all, wts, power,
    t_sem, own_sem, x_send, relay_send, x_recv, x_out, part_send, part_recv, stat_send, stat_recv,
):
    dom = lax.axis_index("dom")
    o = lax.axis_index("orient")
    line = n // 2
    a, b = o // 2, o % 2
    mate = a * 2 + (1 - b)
    rows, width = xin_ref.shape[1], xin_ref.shape[2]
    refs, body = t_ref.shape
    groups = n // group
    cols = group * doms * rows
    early = group == 1
    stages = doms.bit_length() - 1
    half = line // 2

    kd = body // 2
    t_copy = pltpu.make_async_copy(
        tall_ref.at[:, :, pl.ds(pl.multiple_of(dom * kd, kd), kd)], t_raw, t_sem
    )
    t_copy.start()

    barrier = pltpu.get_barrier_semaphore()

    @pl.loop(1, doms)
    def _(i):
        pl.semaphore_signal(barrier, inc=1, device_id=(lax.rem(dom + i, doms), o), device_id_type=MESH)

    @pl.loop(1, n)
    def _(i):
        pl.semaphore_signal(barrier, inc=1, device_id=(dom, lax.rem(o + i, n)), device_id_type=MESH)

    xin_ref[:, :, body:] = jnp.broadcast_to(seen_ref[...][None], (doms, rows, LANES))
    tiled = jnp.concatenate([seen_ref[...]] * (kd // LANES), axis=1)
    for d in range(doms):
        for c in range(2):
            xin_ref[d, :, c * kd:(c + 1) * kd] = raw_ref[:, c, d * kd:(d + 1) * kd] * tiled

    pl.semaphore_wait(barrier, doms + n - 2)

    def spread(i):
        to = lax.rem(dom + i, doms)
        return pltpu.make_async_remote_copy(
            src_ref=xin_ref.at[to], dst_ref=x.at[o, dom],
            send_sem=x_out.at[i], recv_sem=x_recv.at[o, dom],
            device_id=(to, o), device_id_type=MESH,
        )

    own = pltpu.make_async_copy(xin_ref.at[dom], x.at[o, dom], own_sem)
    own.start()
    for i in range(1, doms):
        spread(i).start()

    def hop(direction, p, d, to):
        return pltpu.make_async_remote_copy(
            src_ref=x.at[p, d], dst_ref=x.at[p, d],
            send_sem=x_send.at[direction, p // 2, d], recv_sem=x_recv.at[p, d],
            device_id=(dom, to), device_id_type=MESH,
        )

    def arrive(p, d):
        hop(0, p, d, mate).wait_recv()

    def right(p, d):
        @pl.when(a + 1 < line)
        def _():
            hop(0, p, d, o + 2).start()

    def left(p, d):
        @pl.when(a > 0)
        def _():
            hop(1, p, d, o - 2).start()

    def relayed(at, q, i):
        late = i >= doms // 2
        inner = ((q == at + 1) & (at >= half) & (at < line - 1)) | ((q == at - 1) & (at < half) & (at > 0))
        outer = ((q == at - 1) & (at == line - 1)) | ((q == at + 1) & (at == 0))
        return (inner | outer) if late else inner

    def across(p, d, i):
        @pl.when(jnp.logical_not(relayed(a, p // 2, i)))
        def _():
            hop(2, p, d, mate).start()

    def relay(d, i):
        for sign in (1, -1):
            @pl.when((a + sign >= 0) & (a + sign < line) & relayed(a + sign, a, i))
            def _():
                relay_copy(sign, d).start()

    def relay_copy(sign, d):
        return pltpu.make_async_remote_copy(
            src_ref=x.at[mate, d], dst_ref=x.at[mate, d],
            send_sem=relay_send.at[(1 - sign) // 2, d], recv_sem=x_recv.at[mate, d],
            device_id=(dom, o + 2 * sign), device_id_type=MESH,
        )

    def from_mate(s):
        for sign in (-1, 1):
            @pl.when((a + sign * s >= 0) & (a + sign * s < line))
            def _():
                p = mate + 2 * sign * s
                for i in range(doms):
                    arrive(p, lax.rem(dom + i, doms))
                if early:
                    scores_of(p)

    def part_copy(g, k):
        step = 2 ** k
        flip = dom + step - 2 * step * (dom // step % 2)
        return pltpu.make_async_remote_copy(
            src_ref=part.at[2 * k, g], dst_ref=part.at[2 * k + 1, g],
            send_sem=part_send.at[k, g], recv_sem=part_recv.at[k, g],
            device_id=(flip, o), device_id_type=MESH,
        )

    def power_of():
        total = jnp.zeros((refs, LANES), jnp.float32)
        for j in range(body // LANES):
            piece = t_ref[:, j * LANES:(j + 1) * LANES].astype(jnp.float32)
            total = total + piece * piece
        total = total * -0.5
        high = total.astype(jnp.bfloat16)
        rest = total - high.astype(jnp.float32)
        middle = rest.astype(jnp.bfloat16)
        low = (rest - middle.astype(jnp.float32)).astype(jnp.bfloat16)
        power[0], power[1], power[2] = high, middle, low

    nt = (((1,), (1,)), ((), ()))

    def scores_of(g):
        block = x[pl.ds(g * group, group)].reshape(cols, width)
        seen = block[:, body:]
        total = lax.dot_general(t_ref[...], block[:, :body], nt, preferred_element_type=jnp.float32)
        for j in range(3):
            total = total + lax.dot_general(power[j], seen, nt, preferred_element_type=jnp.float32)
        part[0, g] = total
        part_copy(g, 0).start()
        for k in range(1, stages):
            part_copy(g, k - 1).wait_recv()
            part[2 * k, g] = part[2 * k - 2, g] + part[2 * k - 1, g]
            part_copy(g, k).start()

    own.wait()
    for i in range(doms):
        d = lax.rem(dom + i, doms)
        if i > 0:
            arrive(o, d)
        right(o, d)
        left(o, d)
        across(o, d, i)
    t_copy.wait()
    step = 32

    @pl.loop(0, refs // step)
    def _(j):
        at = pl.ds(pl.multiple_of(j * step, step), step)
        for c in range(2):
            t_ref[at, c * kd:(c + 1) * kd] = t_raw[at, c, :]

    power_of()
    if early:
        scores_of(o)

    @pl.loop(1, line)
    def _(s):
        for i in range(doms):
            d = lax.rem(dom + i, doms)

            @pl.when(a - s >= 0)
            def _():
                p = o - 2 * s
                arrive(p, d)
                right(p, d)
                across(p, d, i)

            @pl.when(a + s < line)
            def _():
                p = o + 2 * s
                arrive(p, d)
                left(p, d)
                across(p, d, i)

        if early:
            for sign in (-1, 1):
                @pl.when((a + sign * s >= 0) & (a + sign * s < line))
                def _():
                    scores_of(o + 2 * sign * s)

        @pl.when(s == 1)
        def _():
            for i in range(doms):
                d = lax.rem(dom + i, doms)
                arrive(mate, d)
                relay(d, i)
            if early:
                scores_of(mate)

        @pl.when(s > 1)
        def _():
            from_mate(s - 1)

    from_mate(line - 1)

    if not early:
        @pl.loop(0, groups)
        def _(g):
            scores_of(g)

    @pl.loop(0, groups)
    def _(g):
        part_copy(g, stages - 1).wait_recv()
        total = part[2 * stages - 2, g] + part[2 * stages - 1, g]
        total = total * scale
        score[g] = total
        peak = jnp.max(total, axis=0, keepdims=True)
        stat[0, pl.ds(g, 1), :] = peak
        stat[1, pl.ds(g, 1), :] = jnp.sum(jnp.exp(total - peak), axis=0, keepdims=True)

    def stat_copy(i):
        return pltpu.make_async_remote_copy(
            src_ref=stat, dst_ref=stat_all.at[o],
            send_sem=stat_send.at[i], recv_sem=stat_recv.at[o],
            device_id=(dom, lax.rem(o + i, n)), device_id_type=MESH,
        )

    @pl.loop(1, n)
    def _(i):
        stat_copy(i).start()

    stat_all[o] = stat[...]

    @pl.loop(1, n)
    def _(i):
        p = lax.rem(o + i, n)
        pltpu.make_async_remote_copy(
            src_ref=stat, dst_ref=stat_all.at[p],
            send_sem=stat_send.at[i], recv_sem=stat_recv.at[p],
            device_id=(dom, p), device_id_type=MESH,
        ).wait_recv()

    top = stat_all[0, 0]
    for p in range(1, n):
        top = jnp.maximum(top, stat_all[p, 0])
    mass = jnp.zeros_like(top)
    for p in range(n):
        mass = mass + stat_all[p, 1] * jnp.exp(stat_all[p, 0] - top)
    lse_ref[...] = top + jnp.log(mass)

    for g in range(groups):
        wts[:, g * cols:(g + 1) * cols] = jnp.exp(score[g] - lse_ref[g:g + 1, :]).astype(jnp.bfloat16)

    nn = (((1,), (0,)), ((), ()))
    seen = x[:, :, :, body:].reshape(n * doms * rows, LANES)
    norm = 1.0 / (lax.dot_general(wts[...], seen, nn, preferred_element_type=jnp.float32) + 1.0)
    tile = 4 * LANES
    norm = jnp.concatenate([norm] * 4, axis=1)

    @pl.loop(0, body // tile)
    def _(j):
        at = pl.ds(pl.multiple_of(j * tile, tile), tile)
        piece = x[:, :, :, at].reshape(n * doms * rows, tile)
        num = lax.dot_general(wts[...], piece, nn, preferred_element_type=jnp.float32)
        out_ref[:, at] = (num + t_ref[:, at].astype(jnp.float32)) * norm

    for i in range(1, doms):
        spread(i).wait_send()

    @pl.loop(0, line)
    def _(q):
        p = q * 2 + b
        for i in range(doms):
            d = lax.rem(dom + i, doms)

            @pl.when((q <= a) & (a + 1 < line))
            def _():
                hop(0, p, d, mate).wait_send()

            @pl.when((q >= a) & (a > 0))
            def _():
                hop(1, p, d, mate).wait_send()

            @pl.when(jnp.logical_not(relayed(a, q, i)))
            def _():
                hop(2, p, d, mate).wait_send()

    for i in range(doms):
        d = lax.rem(dom + i, doms)
        for sign in (1, -1):
            @pl.when((a + sign >= 0) & (a + sign < line) & relayed(a + sign, a, i))
            def _():
                relay_copy(sign, d).wait_send()

    @pl.loop(0, groups)
    def _(g):
        for k in range(stages):
            part_copy(g, k).wait_send()

    @pl.loop(1, n)
    def _(i):
        stat_copy(i).wait_send()


def on_device(particles, templates, tilt_low, tilt_high):
    doms, n = lax.axis_size("dom"), lax.axis_size("orient")
    rows, _, band = particles.shape
    refs = templates.shape[0]
    part_band = band // doms
    body = 2 * part_band
    width = body + LANES
    group = max(1, 2 * LANES // (doms * rows))
    groups = n // group
    cols = group * doms * rows
    stages = doms.bit_length() - 1

    binned = bin_index(jnp.arange(LANES, dtype=jnp.int32))
    seen = (
        (tilt_low[:, None] <= binned[None, :]) & (binned[None, :] < tilt_high[:, None])
    ).astype(jnp.bfloat16)
    vmem = pl.BlockSpec(memory_space=pltpu.VMEM)
    updated, lse = pl.pallas_call(
        functools.partial(kernel, doms, n, group, 3.0 / math.sqrt(band)),
        out_shape=(
            jax.ShapeDtypeStruct((refs, body), jnp.float32),
            jax.ShapeDtypeStruct((groups, cols), jnp.float32),
        ),
        in_specs=[vmem, vmem, pl.BlockSpec(memory_space=pl.ANY)],
        out_specs=(vmem, vmem),
        scratch_shapes=[
            pltpu.VMEM((doms, rows, width), jnp.bfloat16),
            pltpu.VMEM((refs, 2, part_band), jnp.bfloat16),
            pltpu.VMEM((refs, body), jnp.bfloat16),
            pltpu.VMEM((n, doms, rows, width), jnp.bfloat16),
            pltpu.VMEM((2 * stages, groups, refs, cols), jnp.float32),
            pltpu.VMEM((groups, refs, cols), jnp.float32),
            pltpu.VMEM((2, groups, cols), jnp.float32),
            pltpu.VMEM((n, 2, groups, cols), jnp.float32),
            pltpu.VMEM((refs, n * doms * rows), jnp.bfloat16),
            pltpu.VMEM((3, refs, LANES), jnp.bfloat16),
            pltpu.SemaphoreType.DMA,
            pltpu.SemaphoreType.DMA,
            pltpu.SemaphoreType.DMA((3, n // 2, doms)),
            pltpu.SemaphoreType.DMA((2, doms)),
            pltpu.SemaphoreType.DMA((n, doms)),
            pltpu.SemaphoreType.DMA((doms,)),
            pltpu.SemaphoreType.DMA((stages, groups)),
            pltpu.SemaphoreType.DMA((stages, groups)),
            pltpu.SemaphoreType.DMA((n,)),
            pltpu.SemaphoreType.DMA((n,)),
        ],
        compiler_params=pltpu.CompilerParams(
            collective_id=0, has_side_effects=True, vmem_limit_bytes=60 * 2**20
        ),
    )(particles, seen, templates)
    mine = lax.dynamic_index_in_dim(
        lse.reshape(n, doms, rows), lax.axis_index("dom"), 1, keepdims=False
    )
    return updated.reshape(refs, 2, part_band), mine.reshape(n * rows)


def solution(mesh):
    in_specs = (
        P(("dom", "orient"), None, None),
        P("orient", None, None),
        P(("dom", "orient")),
        P(("dom", "orient")),
    )
    out_specs = (P("orient", None, "dom"), P("dom"))
    return jax.shard_map(
        on_device, mesh=mesh, in_specs=in_specs, out_specs=out_specs, check_vma=False
    )
```
